128 devices in a mesh: dom: 8 (over x, core), grp: 16 (over z, y).
Axes of the slice: x: 4, y: 4, z: 4, core: 2. Of those that a mesh axis runs over, the one named last changes fastest.
Arguments:
- features: bfloat16 [524288, 256], P(('dom', 'grp')), may hold values from -6 to 6
- w_fine: bfloat16 [256, 256], replicated, may hold values from -0.375 to 0.375
- adj_tiles: bfloat16 [4096, 20, 128, 128], P(('dom', 'grp')), may hold values from -0.125 to 0.125
- tile_cols: int32 [4096, 20], P(('dom', 'grp')), may hold values from 0 to 39
- tile_count: int32 [4096], P(('dom', 'grp')), may hold values from 1 to 20, as said below
- send_lower: int32 [512], P(('dom', 'grp')), may hold values from 0 to 31
- send_upper: int32 [512], P(('dom', 'grp')), may hold values from 0 to 31
- assign: int32 [524288], P(('dom', 'grp')), may hold values from 0 to 1023, as said below
- w_coarse: bfloat16 [256, 256], replicated, may hold values from -0.375 to 0.375
- coarse_adj: bfloat16 [1024, 1024], P(('dom', 'grp')), may hold values from -0.1875 to 0.1875
Outputs:
- output: bfloat16 [524288, 256], P(('dom', 'grp'))
The draws below stay inside these ranges and needn't reach their ends.
Inputs may be any that keep to these rules, and one draw needn't show every extreme that they name: The first tile_count[r] slots of block row r are live; the others are ignored. `assign`: every coarse node is the coarse node of at least one vertex.
All inputs are finite; a program needn't handle non-finite values.
Results may differ from the reference program's by a relative error of at most 0.011.
Values may be sent and summed in bfloat16 or wider, within the bound.
A program may use at most 192 MiB of HBM per device.

```python
import jax
import jax.numpy as jnp
from jax import lax

F = 256
BS = 128
K = 20
H = 4
NC = 1024
V_DEV = 4096
NB = 32
NBLK = 4096
VERT = 524288
N_DOM = 8
N_GRP = 16
DEVICES = 128


def draw_tile_count(key, part):
    device_count = NBLK // NB
    key_caps, key_draw, key_star = jax.random.split(key, 3)
    device_caps = jax.random.randint(key_caps, (device_count,), 1, K + 1)
    busiest = jax.random.randint(key_star, (), 0, device_count)
    device_caps = device_caps.at[busiest].set(K)
    raw_draw = jax.random.randint(key_draw, (device_count, NB), 0, K)
    counts = 1 + raw_draw % device_caps[:, None]
    counts = counts.at[busiest, 0].set(K)
    return counts.reshape(NBLK).astype(jnp.int32)


def draw_assign(key, part):
    device_count = VERT // V_DEV
    per_device = NC // device_count
    key_spread = jax.random.fold_in(key, 7)
    position = jnp.arange(VERT, dtype=jnp.int32)
    owner_part = position // V_DEV
    within = position % V_DEV
    spread_node = jax.random.randint(key_spread, (VERT,), 0, NC)
    chosen = jnp.where(within < per_device, owner_part * per_device + within, spread_node)
    return chosen.astype(jnp.int32)


def set_ends(entries, rng, smallest, largest):
    longest = entries.shape.index(max(entries.shape))
    spots = []
    for shift in (0, 1):
        where = [jax.random.randint(jax.random.fold_in(rng, axis), (), 0, length) for axis, length in enumerate(entries.shape)]
        where[longest] = (where[longest] + shift) % entries.shape[longest]
        spots.append(tuple(where))
    return entries.at[spots[0]].set(smallest).at[spots[1]].set(largest)


def block_levels(own_key, dims, shards, low, largest):
    factor_of = 1.0
    for dim, shards_of in shards:
        draws = jax.random.uniform(jax.random.fold_in(jax.random.fold_in(own_key, 6), dim), (shards_of,), jnp.float32, low / len(shards), largest / len(shards))
        factor_of = factor_of * jnp.repeat(jnp.exp(draws), dims[dim] // shards_of).reshape((-1,) + (1,) * (len(dims) - 1 - dim))
    return factor_of


def scatter_about(key, shape, deviation, most, pieces=(), kind=jnp.bfloat16):
    level = block_levels(key, shape, pieces, -0.22, 0.18) if pieces else 1.0
    values = jax.random.normal(key, shape, jnp.float32) * deviation * level
    return jnp.minimum(jnp.maximum(values, -most), most).astype(kind)


def setup_inputs(seed: int = 0) -> dict:
    seeds = jax.random.split(jax.random.key(seed), 11)
    return {
        "features": scatter_about(seeds[0], (VERT, F), 1.0, 6.0, ((0, 128),)),
        "w_fine": scatter_about(seeds[1], (F, F), F ** -0.5, 0.375),
        "adj_tiles": scatter_about(seeds[2], (NBLK, K, BS, BS), (K * BS) ** -0.5, 0.125, ((0, 128),)),
        "tile_cols": set_ends(jax.random.randint(seeds[3], (NBLK, K), 0, NB + 2 * H), jax.random.fold_in(seeds[3], 1), 0, (NB + 2 * H) - 1).astype(jnp.int32),
        "tile_count": draw_tile_count(jax.random.fold_in(seeds[10], 71), 0),
        "send_lower": set_ends(jax.random.randint(seeds[5], (DEVICES * H,), 0, NB), jax.random.fold_in(seeds[5], 1), 0, NB - 1).astype(jnp.int32),
        "send_upper": set_ends(jax.random.randint(seeds[6], (DEVICES * H,), 0, NB), jax.random.fold_in(seeds[6], 1), 0, NB - 1).astype(jnp.int32),
        "assign": draw_assign(jax.random.fold_in(seeds[10], 71), 0),
        "w_coarse": scatter_about(seeds[8], (F, F), F ** -0.5, 0.375),
        "coarse_adj": scatter_about(seeds[9], (NC, NC), NC ** -0.5, 0.1875, ((0, 128),)),
    }


def device_spmm(operands):
    extended, weights, columns, live_count = operands
    live_mask = jnp.arange(K)[None, :] < live_count[:, None]
    kept = jnp.where(live_mask[:, :, None, None], weights.astype(jnp.float32), 0.0)
    picked = extended[columns].astype(jnp.float32)
    return jnp.einsum('rkij,rkjf->rif', kept, picked)

def reference(features, w_fine, adj_tiles, tile_cols, tile_count, send_lower, send_upper, assign, w_coarse, coarse_adj):
    block_count = V_DEV // BS
    device_count = N_DOM * N_GRP
    projected = jnp.dot(features, w_fine, preferred_element_type=jnp.float32).astype(jnp.bfloat16)
    flat_blocks = projected.reshape(device_count * block_count, BS, F)
    offsets = (jnp.arange(device_count, dtype=jnp.int32) * block_count)[:, None]
    lower_sel = flat_blocks[send_lower.reshape(device_count, H) + offsets]
    upper_sel = flat_blocks[send_upper.reshape(device_count, H) + offsets]
    lower_sel = lower_sel.reshape(N_DOM, N_GRP, H, BS, F)
    upper_sel = upper_sel.reshape(N_DOM, N_GRP, H, BS, F)
    from_below = jnp.roll(upper_sel, 1, axis=0)
    from_above = jnp.roll(lower_sel, -1, axis=0)
    own_blocks = projected.reshape(N_DOM, N_GRP, block_count, BS, F)
    extended = jnp.concatenate([own_blocks, from_below, from_above], axis=2)
    extended = extended.reshape(device_count, block_count + 2 * H, BS, F)
    fine_out = lax.map(device_spmm, (extended, adj_tiles.reshape(device_count, block_count, K, BS, BS), tile_cols.reshape(device_count, block_count, K), tile_count.reshape(device_count, block_count)))
    fine_out = fine_out.reshape(V_DEV * device_count, F)
    coarse_sums = jax.ops.segment_sum(features.astype(jnp.float32), assign, num_segments=NC)
    counts = jax.ops.segment_sum(jnp.ones((assign.shape[0],), jnp.float32), assign, num_segments=NC)
    coarse = (coarse_sums / jnp.sqrt(counts)[:, None]).astype(jnp.bfloat16)
    coarse_proj = jnp.dot(coarse, w_coarse, preferred_element_type=jnp.float32).astype(jnp.bfloat16)
    coarse_mixed = (coarse_proj.astype(jnp.float32) + jnp.dot(coarse_adj, coarse_proj, preferred_element_type=jnp.float32)).astype(jnp.bfloat16)
    return jax.nn.relu(fine_out + coarse_mixed[assign].astype(jnp.float32)).astype(jnp.bfloat16)
```

```python
import jax
import jax.numpy as jnp
from jax import lax
from jax.experimental import pallas as pl
from jax.experimental.pallas import tpu as pltpu
from jax.sharding import PartitionSpec as P

MESH = pl.DeviceIdType.MESH
F = 256
BS = 128
K = 20
H = 4
NC = 1024
V = 4096
NB = 32
BF = jnp.bfloat16
F32 = jnp.float32
ADJ_CHUNK = 4
FEAT_CHUNK = 1024
OUT_CHUNK = 512


def ring_hops(d):
    return min(d % 4, -d % 4)


OFFSETS = sorted(
    [
        (ox, oz, oy)
        for ox in range(4)
        for oz in range(4)
        for oy in range(4)
        if (ox, oz, oy) != (0, 0, 0)
    ],
    key=lambda o: -sum(ring_hops(d) for d in o),
)


def wait_bytes(ref, sem):
    pltpu.make_async_copy(ref, ref, sem).wait()


def send(src, dst, ssem, rsem, to):
    pltpu.make_async_remote_copy(
        src, dst, ssem, rsem, device_id=to, device_id_type=MESH
    ).start()


def rows_of(pieces):
    wide = pieces.astype(F32)
    n = wide.shape[0]
    low = wide[:, :8, :].reshape(n * 8, 128)
    high = wide[:, 8:16, :].reshape(n * 8, 128)
    return jnp.concatenate([low, high], axis=1)


def piece_of(rows):
    return jnp.concatenate([rows[:, :128], rows[:, 128:]], axis=0).astype(BF)


def kernel(
    feat_hbm, wf_ref, adj_hbm, pick_ref, lower_ref, upper_ref, assign_ref, wc_ref,
    cadj_ref, out_hbm,
    feat, adj, ext, fine, onehot, acol, out, half, hits, core_send, core_recv, rs_send, rs_recv,
    halo, gath, own_piece, table,
    feat_sem, adj_sem, out_sem, core_sems, rs_sems, halo_sems, ag_sems,
):
    dom = lax.axis_index("dom")
    grp = lax.axis_index("grp")
    x, core = dom // 2, dom % 2
    z, y = grp // 4, grp % 4
    chip = x * 16 + grp
    place = dom * 16 + grp

    def chip_at(o):
        return (x + o[0]) % 4, ((z + o[1]) % 4) * 4 + (y + o[2]) % 4

    def same_core(o):
        to_x, to_grp = chip_at(o)
        return {"dom": to_x * 2 + core, "grp": to_grp}

    partner = {"dom": x * 2 + 1 - core, "grp": grp}
    upper = {"dom": (dom + 1) % 8, "grp": grp}
    lower = {"dom": (dom + 7) % 8, "grp": grp}
    across = {"dom": (dom + core * 2 + 7) % 8, "grp": grp}

    feat_copies = []
    for i in range(V // FEAT_CHUNK):
        part = pl.ds(i * FEAT_CHUNK // BS, FEAT_CHUNK // BS)
        c = pltpu.make_async_copy(feat_hbm.at[part], feat.at[part], feat_sem.at[i])
        c.start()
        feat_copies.append(c)
    barrier = pltpu.get_barrier_semaphore()
    for o in OFFSETS:
        pl.semaphore_signal(barrier, inc=1, device_id=same_core(o), device_id_type=MESH)
    pl.semaphore_signal(barrier, inc=1, device_id=partner, device_id_type=MESH)
    pl.semaphore_signal(barrier, inc=1, device_id=across, device_id_type=MESH)
    adj_copies = []
    for i in range(NB // ADJ_CHUNK):
        part = pl.ds(i * ADJ_CHUNK, ADJ_CHUNK)
        c = pltpu.make_async_copy(adj_hbm.at[part], adj.at[part], adj_sem.at[i])
        c.start()
        adj_copies.append(c)

    nodes = assign_ref[...]

    def segment_half(which, arrive):
        local = jnp.where(
            (nodes // 128) % 2 == which, (nodes // 256) * 128 + nodes % 128, -1
        )
        half[...] = jnp.zeros_like(half)
        hits[...] = jnp.zeros_like(hits)
        acol[0, 0:32, :] = local
        for i in range(V // FEAT_CHUNK):
            if arrive:
                feat_copies[i].wait()

            def strip(m, carry):
                base = m * 128
                seat = lax.broadcasted_iota(jnp.int32, (128, 128), 0) + base
                total = jnp.zeros((128, F), F32)
                count = jnp.zeros((128, 128), BF)
                for t in range(FEAT_CHUNK // 256):
                    pair = []
                    for s in range(2):
                        row = i * (FEAT_CHUNK // 128) + 2 * t + s
                        hit = jnp.where(acol[0, row : row + 1, :] == seat, 1.0, 0.0).astype(BF)
                        count = count + hit
                        pair.append(hit)
                    start = i * FEAT_CHUNK + t * 256
                    total = total + jnp.dot(
                        jnp.concatenate(pair, axis=1),
                        feat[pl.ds(start // BS, 2)].reshape(256, F),
                        preferred_element_type=F32,
                    )
                part = pl.ds(pl.multiple_of(base, 128), 128)
                half[part, :] += total
                hits[part, :] += count
                return carry

            lax.fori_loop(0, 4, strip, 0)
        counts = jnp.dot(hits[...], jnp.ones((128, 128), BF), preferred_element_type=F32)
        sums = half[...].reshape(64, 8, F)
        return jnp.concatenate(
            [sums[:, :, :128], sums[:, :, 128:], counts.reshape(64, 8, 128)], axis=1
        )

    core_send[...] = segment_half(1 - core, True).astype(BF)
    pl.semaphore_wait(barrier, len(OFFSETS) + 2)
    send(core_send, core_recv, core_sems.at[0], core_sems.at[1], partner)
    mine = segment_half(core, False)
    wait_bytes(core_recv, core_sems.at[1])
    rs_send[...] = (mine + core_recv[...].astype(F32)).astype(BF)
    for o in OFFSETS:
        to_x, to_grp = chip_at(o)
        send(
            rs_send.at[to_x * 16 + to_grp], rs_recv.at[chip], rs_sems.at[0], rs_sems.at[1],
            same_core(o),
        )
    rs_recv[chip] = rs_send[chip]

    for i in range(H):
        for side, ref in enumerate((lower_ref, upper_ref)):
            block = feat[ref[i]]
            halo[side, i] = jnp.dot(block, wf_ref[...], preferred_element_type=F32).astype(BF)
    send(halo.at[0], ext.at[pl.ds(NB + H, H)], halo_sems.at[0], halo_sems.at[1], lower)
    send(halo.at[1], ext.at[pl.ds(NB, H)], halo_sems.at[2], halo_sems.at[3], upper)

    def project(i, carry):
        block = feat[pl.ds(i * 4, 4)].reshape(512, F)
        rows = jnp.dot(block, wf_ref[...], preferred_element_type=F32).astype(BF)
        ext[pl.ds(i * 4, 4)] = rows.reshape(4, BS, F)
        return carry

    lax.fori_loop(0, V // 512, project, 0)
    ext[NB + 2 * H] = jnp.zeros((BS, F), BF)

    turned = nodes.astype(F32).T
    for r in range(NB):
        acol[r] = jnp.broadcast_to(turned[:, r : r + 1], (BS, 128)).astype(jnp.int32)
    lanes = lax.broadcasted_iota(jnp.int32, (BS, 128), 1)

    def spread(r, carry):
        col = acol[r]
        for j in range(NC // 128):
            hit = jnp.where(col == lanes + j * 128, 1.0, 0.0).astype(BF)
            onehot[pl.ds(pl.multiple_of(r * BS, BS), BS), j * 128 : (j + 1) * 128] = hit
        return carry

    lax.fori_loop(0, NB, spread, 0)

    def spmm(r, carry):
        total = jnp.zeros((BS, F), F32)
        for k in range(0, K, 2):
            tiles = jnp.concatenate([adj[r, k], adj[r, k + 1]], axis=1)
            blocks = jnp.concatenate([ext[pick_ref[r, k]], ext[pick_ref[r, k + 1]]], axis=0)
            total = total + jnp.dot(tiles, blocks, preferred_element_type=F32)
        fine[pl.ds(pl.multiple_of(r * BS, BS), BS), :] = total
        return carry

    def gather_all(step, piece):
        buf = gath.at[step]
        own_piece[step] = piece
        buf[place] = piece
        for o in OFFSETS:
            send(
                own_piece.at[step], buf.at[place], ag_sems.at[step, 0], ag_sems.at[step, 1],
                same_core(o),
            )

    def gather_cores(step):
        buf = gath.at[step]
        wait_bytes(buf.at[pl.ds(0, 63)], ag_sems.at[step, 1])
        for i in range(4):
            part = buf.at[pl.ds(i * 32 + core * 16, 16)]
            send(part, part, ag_sems.at[step, 2], ag_sems.at[step, 3], partner)
        wait_bytes(buf.at[pl.ds(0, 64)], ag_sems.at[step, 3])

    wait_bytes(rs_recv.at[pl.ds(0, 63)], rs_sems.at[1])
    whole = jnp.sum(rs_recv[...].astype(F32), axis=0)
    root = jnp.sqrt(whole[16:24, :])
    coarse = jnp.concatenate([whole[:8, :] / root, whole[8:16, :] / root], axis=1).astype(BF)
    projected = jnp.dot(coarse, wc_ref[...], preferred_element_type=F32)
    gather_all(0, piece_of(projected))

    wait_bytes(ext.at[pl.ds(NB, H)], halo_sems.at[1])
    wait_bytes(ext.at[pl.ds(NB, H)], halo_sems.at[3])
    for i in range(4):
        adj_copies[i].wait()
    lax.fori_loop(0, 16, spmm, 0)

    gather_cores(0)
    mixed = jnp.dot(cadj_ref[...], rows_of(gath[0]).astype(BF), preferred_element_type=F32)
    gather_all(1, piece_of(mixed + projected.astype(BF).astype(F32)))

    for i in range(4, 8):
        adj_copies[i].wait()
    lax.fori_loop(16, 32, spmm, 0)

    gather_cores(1)
    table[...] = rows_of(gath[1]).astype(BF)

    for i in range(V // OUT_CHUNK):
        part = pl.ds(i * OUT_CHUNK, OUT_CHUNK)
        got = jnp.dot(onehot[part, :], table[...], preferred_element_type=F32)
        out[part, :] = jnp.maximum(fine[part, :] + got, 0.0).astype(BF)
        pltpu.make_async_copy(out.at[part], out_hbm.at[part], out_sem.at[i]).start()

    wait_bytes(core_send, core_sems.at[0])
    wait_bytes(rs_send.at[pl.ds(0, 63)], rs_sems.at[0])
    wait_bytes(halo.at[0], halo_sems.at[0])
    wait_bytes(halo.at[1], halo_sems.at[2])
    for step in range(2):
        wait_bytes(gath.at[step, pl.ds(0, 63)], ag_sems.at[step, 0])
        wait_bytes(gath.at[step, pl.ds(0, 64)], ag_sems.at[step, 2])
    for i in range(V // OUT_CHUNK):
        part = pl.ds(i * OUT_CHUNK, OUT_CHUNK)
        pltpu.make_async_copy(out.at[part], out_hbm.at[part], out_sem.at[i]).wait()


def per_device(
    features, w_fine, adj_tiles, tile_cols, tile_count, send_lower, send_upper, assign, w_coarse,
    coarse_adj,
):
    vmem = pl.BlockSpec(memory_space=pltpu.VMEM)
    smem = pl.BlockSpec(memory_space=pltpu.SMEM)
    hbm = pl.BlockSpec(memory_space=pl.ANY)
    dma = pltpu.SemaphoreType.DMA
    pick = jnp.where(jnp.arange(K)[None, :] < tile_count[:, None], tile_cols, NB + 2 * H)
    return pl.pallas_call(
        kernel,
        out_shape=jax.ShapeDtypeStruct((V, F), BF),
        in_specs=[hbm, vmem, hbm, smem, smem, smem, vmem, vmem, vmem],
        out_specs=hbm,
        scratch_shapes=[
            pltpu.VMEM((NB, BS, F), BF),
            pltpu.VMEM((NB, K, BS, BS), BF),
            pltpu.VMEM((NB + 2 * H + 1, BS, F), BF),
            pltpu.VMEM((V, F), F32),
            pltpu.VMEM((V, NC), BF),
            pltpu.VMEM((NB, BS, 128), jnp.int32),
            pltpu.VMEM((V, F), BF),
            pltpu.VMEM((NC // 2, F), F32),
            pltpu.VMEM((NC // 2, 128), BF),
            pltpu.VMEM((64, 24, 128), BF),
            pltpu.VMEM((64, 24, 128), BF),
            pltpu.VMEM((64, 24, 128), BF),
            pltpu.VMEM((64, 24, 128), BF),
            pltpu.VMEM((2, H, BS, F), BF),
            pltpu.VMEM((2, 128, 16, 128), BF),
            pltpu.VMEM((2, 16, 128), BF),
            pltpu.VMEM((NC, F), BF),
            dma((V // FEAT_CHUNK,)),
            dma((NB // ADJ_CHUNK,)),
            dma((V // OUT_CHUNK,)),
            dma((2,)),
            dma((2,)),
            dma((4,)),
            dma((2, 4)),
        ],
        compiler_params=pltpu.CompilerParams(
            collective_id=0, has_side_effects=True, vmem_limit_bytes=62 * 1024 * 1024
        ),
    )(
        features.reshape(NB, BS, F), w_fine, adj_tiles, pick, send_lower, send_upper,
        assign.reshape(NB, BS), w_coarse, coarse_adj,
    )


def solution(mesh):
    both = ("dom", "grp")
    placed = (
        P(both, None), P(), P(both, None, None, None), P(both, None), P(both), P(both), P(both),
        P(both), P(), P(both, None),
    )
    return jax.shard_map(
        per_device, mesh=mesh, in_specs=placed, out_specs=P(both, None), check_vma=False
    )
```

```python
import jax
import jax.numpy as jnp
from jax import lax
from jax.experimental import pallas as pl
from jax.experimental.pallas import tpu as pltpu
from jax.sharding import PartitionSpec as P

MESH = pl.DeviceIdType.MESH
F = 256
BS = 128
K = 20
H = 4
NC = 1024
V = 4096
NB = 32
BF = jnp.bfloat16
F32 = jnp.float32
ADJ_CHUNK = 4
FEAT_CHUNK = 1024
OUT_CHUNK = 512
DEAD = NB + 2 * H


def ring_hops(d):
    return min(d % 4, -d % 4)


OFFSETS = sorted(
    [
        (ox, oz, oy)
        for ox in range(4)
        for oz in range(4)
        for oy in range(4)
        if (ox, oz, oy) != (0, 0, 0)
    ],
    key=lambda o: -sum(ring_hops(d) for d in o),
)


def wait_bytes(ref, sem):
    pltpu.make_async_copy(ref, ref, sem).wait()


def send(src, dst, ssem, rsem, to):
    pltpu.make_async_remote_copy(
        src, dst, ssem, rsem, device_id=to, device_id_type=MESH
    ).start()


def rows_of(pieces):
    wide = pieces.astype(F32)
    n = wide.shape[0]
    low = wide[:, :8, :].reshape(n * 8, 128)
    high = wide[:, 8:16, :].reshape(n * 8, 128)
    return jnp.concatenate([low, high], axis=1)


def piece_of(rows):
    return jnp.concatenate([rows[:, :128], rows[:, 128:]], axis=0).astype(BF)


def kernel(
    feat_hbm, wf_ref, adj_hbm, cols_hbm, live_ref, lower_ref, upper_ref, assign_ref, wc_ref,
    cadj_ref, out,
    feat, adj, ext, fine, onehot, acol, low, match, match16, hit, mine, cols, core_send, core_recv, rs_send, rs_recv,
    halo, gath, own_piece, table,
    feat_sem, adj_sem, cols_sem, core_sems, rs_sems, halo_sems, ag_sems,
):
    dom = lax.axis_index("dom")
    grp = lax.axis_index("grp")
    x, core = dom // 2, dom % 2
    z, y = grp // 4, grp % 4
    chip = x * 16 + grp
    place = dom * 16 + grp

    def chip_at(o):
        return (x + o[0]) % 4, ((z + o[1]) % 4) * 4 + (y + o[2]) % 4

    def same_core(o):
        to_x, to_grp = chip_at(o)
        return {"dom": to_x * 2 + core, "grp": to_grp}

    partner = {"dom": x * 2 + 1 - core, "grp": grp}
    upper = {"dom": (dom + 1) % 8, "grp": grp}
    lower = {"dom": (dom + 7) % 8, "grp": grp}
    across = {"dom": (dom + core * 2 + 7) % 8, "grp": grp}

    feat_copies = []
    for i in range(V // FEAT_CHUNK):
        part = pl.ds(i * FEAT_CHUNK // BS, FEAT_CHUNK // BS)
        c = pltpu.make_async_copy(feat_hbm.at[part], feat.at[part], feat_sem.at[i])
        c.start()
        feat_copies.append(c)
    barrier = pltpu.get_barrier_semaphore()
    for o in OFFSETS:
        pl.semaphore_signal(barrier, inc=1, device_id=same_core(o), device_id_type=MESH)
    pl.semaphore_signal(barrier, inc=1, device_id=partner, device_id_type=MESH)
    pl.semaphore_signal(barrier, inc=1, device_id=across, device_id_type=MESH)
    cols_copy = pltpu.make_async_copy(cols_hbm, cols, cols_sem)
    cols_copy.start()
    adj_copies = []
    for i in range(NB // ADJ_CHUNK):
        part = pl.ds(i * ADJ_CHUNK, ADJ_CHUNK)
        c = pltpu.make_async_copy(adj_hbm.at[part], adj.at[part], adj_sem.at[i])
        c.start()
        adj_copies.append(c)

    nodes = assign_ref[...]
    low[...] = nodes & 127
    for m in range(NC // 128):
        match[m] = jnp.where((nodes >> 7) == m, 1.0, 0.0)
    seat = lax.broadcasted_iota(jnp.int32, (BS, 128), 0)

    def hits_of(b, carry):
        hit[b] = jnp.where(low[pl.ds(b, 1), :] == seat, 1.0, 0.0).astype(BF)
        for m in range(NC // 128):
            row = match[m, pl.ds(b, 1), :]
            match16[m, b] = jnp.broadcast_to(row, (16, 128)).astype(BF)
        return carry

    lax.fori_loop(0, NB, hits_of, 0, unroll=4)
    for c in feat_copies:
        c.wait()

    def segment_half(which, put):
        for g in range(2):
            total = jnp.zeros((256, F), F32)
            counts = [jnp.zeros((128, 128), BF) for _ in range(2)]
            for t in range(V // 256):
                strips = []
                for i in range(2):
                    m = 4 * g + 2 * i + which
                    pair = []
                    for b in (2 * t, 2 * t + 1):
                        one = hit[b] * jnp.concatenate([match16[m, b]] * 8, axis=0)
                        counts[i] = counts[i] + one
                        pair.append(one)
                    strips.append(jnp.concatenate(pair, axis=1))
                total = total + jnp.dot(
                    jnp.concatenate(strips, axis=0),
                    feat[pl.ds(2 * t, 2)].reshape(256, F),
                    preferred_element_type=F32,
                )
            count = jnp.dot(
                jnp.concatenate(counts, axis=0), jnp.ones((128, 128), BF),
                preferred_element_type=F32,
            )
            sums = total.reshape(32, 8, F)
            put(
                pl.ds(32 * g, 32),
                jnp.concatenate(
                    [sums[:, :, :128], sums[:, :, 128:], count.reshape(32, 8, 128)], axis=1
                ),
            )

    def put_send(part, value):
        core_send[part] = value.astype(BF)

    def put_mine(part, value):
        mine[part] = value

    segment_half(1 - core, put_send)
    pl.semaphore_wait(barrier, len(OFFSETS) + 2)
    send(core_send, core_recv, core_sems.at[0], core_sems.at[1], partner)
    segment_half(core, put_mine)
    wait_bytes(core_recv, core_sems.at[1])
    rs_send[...] = (mine[...] + core_recv[...].astype(F32)).astype(BF)
    for o in OFFSETS:
        to_x, to_grp = chip_at(o)
        send(
            rs_send.at[to_x * 16 + to_grp], rs_recv.at[chip], rs_sems.at[0], rs_sems.at[1],
            same_core(o),
        )
    rs_recv[chip] = rs_send[chip]

    for i in range(H):
        for side, ref in enumerate((lower_ref, upper_ref)):
            block = feat[ref[i]]
            halo[side, i] = jnp.dot(block, wf_ref[...], preferred_element_type=F32).astype(BF)
    send(halo.at[0], ext.at[pl.ds(NB + H, H)], halo_sems.at[0], halo_sems.at[1], lower)
    send(halo.at[1], ext.at[pl.ds(NB, H)], halo_sems.at[2], halo_sems.at[3], upper)

    def project(i, carry):
        block = feat[pl.ds(i * 4, 4)].reshape(512, F)
        rows = jnp.dot(block, wf_ref[...], preferred_element_type=F32).astype(BF)
        ext[pl.ds(i * 4, 4)] = rows.reshape(4, BS, F)
        return carry

    lax.fori_loop(0, V // 512, project, 0, unroll=4)
    ext[DEAD] = jnp.zeros((BS, F), BF)

    turned = nodes.astype(F32).T
    for r in range(NB):
        acol[r] = jnp.broadcast_to(turned[:, r : r + 1], (BS, 128)).astype(jnp.int32)
    lanes = lax.broadcasted_iota(jnp.int32, (BS, 128), 1)

    def spread(r, carry):
        apart = acol[r] - lanes
        tile = jnp.where((apart & 127) == 0, apart >> 7, -1).astype(F32).astype(BF)
        one, none = jnp.ones((BS, 128), BF), jnp.zeros((BS, 128), BF)
        for j in range(NC // 128):
            onehot[pl.ds(pl.multiple_of(r * BS, BS), BS), j * 128 : (j + 1) * 128] = jnp.where(
                tile == j, one, none
            )
        return carry

    lax.fori_loop(0, NB, spread, 0, unroll=2)

    def pick(r, k):
        live = jnp.minimum(jnp.maximum(live_ref[r] - k, 0), 1)
        return DEAD + (cols[k, r] - DEAD) * live

    def spmm(r, carry):
        total = jnp.zeros((BS, F), F32)
        for k in range(0, K, 2):
            tiles = jnp.concatenate([adj[r, k], adj[r, k + 1]], axis=1)
            blocks = jnp.concatenate([ext[pick(r, k)], ext[pick(r, k + 1)]], axis=0)
            total = total + jnp.dot(tiles, blocks, preferred_element_type=F32)
        fine[pl.ds(pl.multiple_of(r * BS, BS), BS), :] = total
        return carry

    def gather_all(step, piece):
        buf = gath.at[step]
        own_piece[step] = piece
        buf[place] = piece
        for o in OFFSETS:
            send(
                own_piece.at[step], buf.at[place], ag_sems.at[step, 0], ag_sems.at[step, 1],
                same_core(o),
            )

    def gather_cores(step):
        buf = gath.at[step]
        wait_bytes(buf.at[pl.ds(0, 63)], ag_sems.at[step, 1])
        for i in range(4):
            part = buf.at[pl.ds(i * 32 + core * 16, 16)]
            send(part, part, ag_sems.at[step, 2], ag_sems.at[step, 3], partner)
        wait_bytes(buf.at[pl.ds(0, 64)], ag_sems.at[step, 3])

    wait_bytes(rs_recv.at[pl.ds(0, 63)], rs_sems.at[1])
    whole = jnp.sum(rs_recv[...].astype(F32), axis=0)
    root = jnp.sqrt(whole[16:24, :])
    coarse = jnp.concatenate([whole[:8, :] / root, whole[8:16, :] / root], axis=1).astype(BF)
    projected = jnp.dot(coarse, wc_ref[...], preferred_element_type=F32)
    gather_all(0, piece_of(projected))

    wait_bytes(ext.at[pl.ds(NB, H)], halo_sems.at[1])
    wait_bytes(ext.at[pl.ds(NB, H)], halo_sems.at[3])
    for i in range(4):
        adj_copies[i].wait()
    cols_copy.wait()
    lax.fori_loop(0, 16, spmm, 0, unroll=4)

    gather_cores(0)
    mixed = jnp.dot(cadj_ref[...], rows_of(gath[0]).astype(BF), preferred_element_type=F32)
    gather_all(1, piece_of(mixed + projected.astype(BF).astype(F32)))

    for i in range(4, 8):
        adj_copies[i].wait()
    lax.fori_loop(16, 32, spmm, 0, unroll=4)

    gather_cores(1)
    table[...] = rows_of(gath[1]).astype(BF)

    for i in range(V // OUT_CHUNK):
        part = pl.ds(i * OUT_CHUNK, OUT_CHUNK)
        got = jnp.dot(onehot[part, :], table[...], preferred_element_type=F32)
        out[part, :] = jnp.maximum(fine[part, :] + got, 0.0).astype(BF)

    wait_bytes(core_send, core_sems.at[0])
    wait_bytes(rs_send.at[pl.ds(0, 63)], rs_sems.at[0])
    wait_bytes(halo.at[0], halo_sems.at[0])
    wait_bytes(halo.at[1], halo_sems.at[2])
    for step in range(2):
        wait_bytes(gath.at[step, pl.ds(0, 63)], ag_sems.at[step, 0])
        wait_bytes(gath.at[step, pl.ds(0, 64)], ag_sems.at[step, 2])


def per_device(
    features, w_fine, adj_tiles, tile_cols, tile_count, send_lower, send_upper, assign, w_coarse,
    coarse_adj,
):
    vmem = pl.BlockSpec(memory_space=pltpu.VMEM)
    smem = pl.BlockSpec(memory_space=pltpu.SMEM)
    hbm = pl.BlockSpec(memory_space=pl.ANY)
    dma = pltpu.SemaphoreType.DMA
    return pl.pallas_call(
        kernel,
        out_shape=pltpu.VMEM((V, F), BF),
        in_specs=[hbm, vmem, hbm, hbm, smem, smem, smem, vmem, vmem, vmem],
        out_specs=vmem,
        scratch_shapes=[
            pltpu.VMEM((NB, BS, F), BF),
            pltpu.VMEM((NB, K, BS, BS), BF),
            pltpu.VMEM((NB + 2 * H + 1, BS, F), BF),
            pltpu.VMEM((V, F), F32),
            pltpu.VMEM((V, NC), BF),
            pltpu.VMEM((NB, BS, 128), jnp.int32),
            pltpu.VMEM((NB, 128), jnp.int32),
            pltpu.VMEM((8, NB, 128), F32),
            pltpu.VMEM((8, NB, 16, 128), BF),
            pltpu.VMEM((NB, BS, 128), BF),
            pltpu.VMEM((64, 24, 128), F32),
            pltpu.SMEM((K, NB), jnp.int32),
            pltpu.VMEM((64, 24, 128), BF),
            pltpu.VMEM((64, 24, 128), BF),
            pltpu.VMEM((64, 24, 128), BF),
            pltpu.VMEM((64, 24, 128), BF),
            pltpu.VMEM((2, H, BS, F), BF),
            pltpu.VMEM((2, 128, 16, 128), BF),
            pltpu.VMEM((2, 16, 128), BF),
            pltpu.VMEM((NC, F), BF),
            dma((V // FEAT_CHUNK,)),
            dma((NB // ADJ_CHUNK,)),
            dma,
            dma((2,)),
            dma((2,)),
            dma((4,)),
            dma((2, 4)),
        ],
        compiler_params=pltpu.CompilerParams(
            collective_id=0, has_side_effects=True, vmem_limit_bytes=52 * 1024 * 1024
        ),
    )(
        features.reshape(NB, BS, F), w_fine, adj_tiles, tile_cols.T, tile_count, send_lower, send_upper,
        assign.reshape(NB, BS), w_coarse, coarse_adj,
    )


def solution(mesh):
    both = ("dom", "grp")
    placed = (
        P(both, None), P(), P(both, None, None, None), P(both, None), P(both), P(both), P(both),
        P(both), P(), P(both, None),
    )
    return jax.shard_map(
        per_device, mesh=mesh, in_specs=placed, out_specs=P(both, None), check_vma=False
    )
```

```python
import jax
import jax.numpy as jnp
from jax import lax
from jax.experimental import pallas as pl
from jax.experimental.pallas import tpu as pltpu
from jax.sharding import PartitionSpec as P

MESH = pl.DeviceIdType.MESH
F = 256
BS = 128
K = 20
H = 4
NC = 1024
V = 4096
NB = 32
BF = jnp.bfloat16
F32 = jnp.float32
ADJ_CHUNK = 4
FEAT_CHUNK = 1024
OUT_CHUNK = 512
STRIPS = (
    (0, 384, ("y", "z", "x")), (384, 384, ("z", "x", "y")), (768, 256, ("x", "y", "z")),
)
DEAD = NB + 2 * H


def ring_hops(d):
    return min(d % 4, -d % 4)


OFFSETS = sorted(
    [
        (ox, oz, oy)
        for ox in range(4)
        for oz in range(4)
        for oy in range(4)
        if (ox, oz, oy) != (0, 0, 0)
    ],
    key=lambda o: -sum(ring_hops(d) for d in o),
)


def wait_bytes(ref, sem):
    pltpu.make_async_copy(ref, ref, sem).wait()


def send(src, dst, ssem, rsem, to):
    pltpu.make_async_remote_copy(
        src, dst, ssem, rsem, device_id=to, device_id_type=MESH
    ).start()


def rows_of(pieces):
    wide = pieces.astype(F32)
    n = wide.shape[0]
    low = wide[:, :8, :].reshape(n * 8, 128)
    high = wide[:, 8:16, :].reshape(n * 8, 128)
    return jnp.concatenate([low, high], axis=1)


def piece_of(rows):
    return jnp.concatenate([rows[:, :128], rows[:, 128:]], axis=0).astype(BF)


def kernel(
    feat_hbm, wf_ref, adj_hbm, cols_hbm, live_ref, lower_ref, upper_ref, assign_ref, wc_ref,
    cadj_ref, out,
    feat, adj, ext, fine, onehot, acol, low, match, match16, hit, mine, cols, core_send, core_recv, rs_send, rs_recv,
    halo, gath, own_piece, table, whole_adj,
    feat_sem, adj_sem, cols_sem, core_sems, rs_sems, halo_sems, ag_sems, strip_sems, swap_sems,
):
    dom = lax.axis_index("dom")
    grp = lax.axis_index("grp")
    x, core = dom // 2, dom % 2
    z, y = grp // 4, grp % 4
    chip = x * 16 + grp
    place = dom * 16 + grp

    def chip_at(o):
        return (x + o[0]) % 4, ((z + o[1]) % 4) * 4 + (y + o[2]) % 4

    def same_core(o):
        to_x, to_grp = chip_at(o)
        return {"dom": to_x * 2 + core, "grp": to_grp}

    partner = {"dom": x * 2 + 1 - core, "grp": grp}
    upper = {"dom": (dom + 1) % 8, "grp": grp}
    lower = {"dom": (dom + 7) % 8, "grp": grp}
    across = {"dom": (dom + core * 2 + 7) % 8, "grp": grp}

    feat_copies = []
    for i in range(V // FEAT_CHUNK):
        part = pl.ds(i * FEAT_CHUNK // BS, FEAT_CHUNK // BS)
        c = pltpu.make_async_copy(feat_hbm.at[part], feat.at[part], feat_sem.at[i])
        c.start()
        feat_copies.append(c)
    barrier = pltpu.get_barrier_semaphore()
    for o in OFFSETS:
        pl.semaphore_signal(barrier, inc=1, device_id=same_core(o), device_id_type=MESH)
    pl.semaphore_signal(barrier, inc=1, device_id=partner, device_id_type=MESH)
    pl.semaphore_signal(barrier, inc=1, device_id=across, device_id_type=MESH)
    cols_copy = pltpu.make_async_copy(cols_hbm, cols, cols_sem)
    cols_copy.start()
    adj_copies = []
    for i in range(NB // ADJ_CHUNK):
        part = pl.ds(i * ADJ_CHUNK, ADJ_CHUNK)
        c = pltpu.make_async_copy(adj_hbm.at[part], adj.at[part], adj_sem.at[i])
        c.start()
        adj_copies.append(c)

    whole_adj[x, core, z, y] = cadj_ref[...]
    spot = {"x": x, "z": z, "y": y}

    def region(free, strip, most=None):
        at = [pl.ds(0, 4) if a in free else spot[a] for a in ("x", "z", "y")]
        return whole_adj.at[at[0], core, at[1], at[2], :, pl.ds(strip[0], strip[1])]

    def strips_go(stage):
        for i, strip in enumerate(STRIPS):
            free, axis = strip[2][:stage], strip[2][stage]
            part = region(free, strip)
            for step in (2, 1, 3):
                o = [step if a == axis else 0 for a in ("x", "z", "y")]
                send(part, part, strip_sems.at[i, stage, 0], strip_sems.at[i, stage, 1], same_core(o))

    def strips_wait(stage, way):
        for i, strip in enumerate(STRIPS):
            cut = pl.ds(strip[0], strip[1])
            if stage == 0:
                three = whole_adj.at[0, 0, 0, pl.ds(0, 3), :, cut]
            elif stage == 1:
                three = whole_adj.at[0, 0, pl.ds(0, 3), pl.ds(0, 4), :, cut]
            else:
                three = whole_adj.at[pl.ds(0, 3), 0, pl.ds(0, 4), pl.ds(0, 4), :, cut]
            wait_bytes(three, strip_sems.at[i, stage, way])

    def halo_parts(part):
        first = part * (H // 2)
        for side, base in ((0, NB + H), (1, NB)):
            yield side, pl.ds(first, H // 2), pl.ds(base + first, H // 2)

    def halo_go(part):
        for side, src, dst in halo_parts(part):
            send(
                halo.at[side, src], ext.at[dst], halo_sems.at[part, side, 0],
                halo_sems.at[part, side, 1], (lower, upper)[side],
            )

    def halo_wait(way):
        for part in range(2):
            for side, src, dst in halo_parts(part):
                wait_bytes(ext.at[dst], halo_sems.at[part, side, way])

    nodes = assign_ref[...]
    low[...] = nodes & 127
    for m in range(NC // 128):
        match[m] = jnp.where((nodes >> 7) == m, 1.0, 0.0)
    seat = lax.broadcasted_iota(jnp.int32, (BS, 128), 0)

    def hits_of(b, carry):
        hit[b] = jnp.where(low[pl.ds(b, 1), :] == seat, 1.0, 0.0).astype(BF)
        for m in range(NC // 128):
            row = match[m, pl.ds(b, 1), :]
            match16[m, b] = jnp.broadcast_to(row, (16, 128)).astype(BF)
        return carry

    lax.fori_loop(0, NB, hits_of, 0, unroll=4)
    for c in feat_copies:
        c.wait()

    def segment_half(which, put):
        for g in range(2):
            total = jnp.zeros((256, F), F32)
            counts = [jnp.zeros((128, 128), BF) for _ in range(2)]
            for t in range(V // 256):
                strips = []
                for i in range(2):
                    m = 4 * g + 2 * i + which
                    pair = []
                    for b in (2 * t, 2 * t + 1):
                        one = hit[b] * jnp.concatenate([match16[m, b]] * 8, axis=0)
                        counts[i] = counts[i] + one
                        pair.append(one)
                    strips.append(jnp.concatenate(pair, axis=1))
                total = total + jnp.dot(
                    jnp.concatenate(strips, axis=0),
                    feat[pl.ds(2 * t, 2)].reshape(256, F),
                    preferred_element_type=F32,
                )
            count = jnp.dot(
                jnp.concatenate(counts, axis=0), jnp.ones((128, 128), BF),
                preferred_element_type=F32,
            )
            sums = total.reshape(32, 8, F)
            put(
                pl.ds(32 * g, 32),
                jnp.concatenate(
                    [sums[:, :, :128], sums[:, :, 128:], count.reshape(32, 8, 128)], axis=1
                ),
            )

    def put_send(part, value):
        core_send[part] = value.astype(BF)

    def put_mine(part, value):
        mine[part] = value

    segment_half(1 - core, put_send)
    for i in range(H):
        for side, ref in enumerate((lower_ref, upper_ref)):
            block = feat[ref[i]]
            halo[side, i] = jnp.dot(block, wf_ref[...], preferred_element_type=F32).astype(BF)
    pl.semaphore_wait(barrier, len(OFFSETS) + 2)
    strips_go(0)
    send(core_send, core_recv, core_sems.at[0], core_sems.at[1], partner)
    halo_go(0)
    segment_half(core, put_mine)
    wait_bytes(core_recv, core_sems.at[1])
    rs_send[...] = (mine[...] + core_recv[...].astype(F32)).astype(BF)
    for o in OFFSETS:
        to_x, to_grp = chip_at(o)
        send(
            rs_send.at[to_x * 16 + to_grp], rs_recv.at[chip], rs_sems.at[0], rs_sems.at[1],
            same_core(o),
        )
    rs_recv[chip] = rs_send[chip]

    def project(i, carry):
        block = feat[pl.ds(i * 4, 4)].reshape(512, F)
        rows = jnp.dot(block, wf_ref[...], preferred_element_type=F32).astype(BF)
        ext[pl.ds(i * 4, 4)] = rows.reshape(4, BS, F)
        return carry

    lax.fori_loop(0, V // 512, project, 0, unroll=4)
    ext[DEAD] = jnp.zeros((BS, F), BF)

    strips_wait(0, 1)
    strips_go(1)
    halo_go(1)
    turned = nodes.astype(F32).T
    for r in range(NB):
        acol[r] = jnp.broadcast_to(turned[:, r : r + 1], (BS, 128)).astype(jnp.int32)
    lanes = lax.broadcasted_iota(jnp.int32, (BS, 128), 1)

    def spread(r, carry):
        apart = acol[r] - lanes
        tile = jnp.where((apart & 127) == 0, apart >> 7, -1).astype(F32).astype(BF)
        one, none = jnp.ones((BS, 128), BF), jnp.zeros((BS, 128), BF)
        for j in range(NC // 128):
            lanes_of = pl.ds(j // 2 * 128, 128)
            onehot[j % 2, pl.ds(pl.multiple_of(r * BS, BS), BS), lanes_of] = jnp.where(
                tile == j, one, none
            )
        return carry

    lax.fori_loop(0, NB, spread, 0, unroll=2)

    def pick(r, k):
        live = jnp.minimum(jnp.maximum(live_ref[r] - k, 0), 1)
        return DEAD + (cols[k, r] - DEAD) * live

    def spmm(r, carry):
        total = jnp.zeros((BS, F), F32)
        for k in range(0, K, 2):
            tiles = jnp.concatenate([adj[r, k], adj[r, k + 1]], axis=1)
            blocks = jnp.concatenate([ext[pick(r, k)], ext[pick(r, k + 1)]], axis=0)
            total = total + jnp.dot(tiles, blocks, preferred_element_type=F32)
        fine[pl.ds(pl.multiple_of(r * BS, BS), BS), :] = total
        return carry

    wait_bytes(rs_recv.at[pl.ds(0, 63)], rs_sems.at[1])
    whole = jnp.sum(rs_recv[...].astype(F32), axis=0)
    root = jnp.sqrt(whole[16:24, :])
    coarse = jnp.concatenate([whole[:8, :] / root, whole[8:16, :] / root], axis=1).astype(BF)
    projected = jnp.dot(coarse, wc_ref[...], preferred_element_type=F32)
    own_piece[...] = piece_of(projected)
    gath[place] = own_piece[...]
    for o in OFFSETS:
        send(own_piece, gath.at[place], ag_sems.at[0], ag_sems.at[1], same_core(o))
    strips_wait(1, 1)
    strips_go(2)
    halo_wait(1)
    for i in range(4):
        adj_copies[i].wait()
    cols_copy.wait()
    lax.fori_loop(0, 16, spmm, 0, unroll=4)

    for i in range(4, 8):
        adj_copies[i].wait()
    lax.fori_loop(16, 32, spmm, 0, unroll=4)
    strips_wait(2, 1)
    wait_bytes(gath.at[pl.ds(0, 63)], ag_sems.at[1])
    for i in range(4):
        part = gath.at[pl.ds(i * 32 + core * 16, 16)]
        send(part, part, ag_sems.at[2], ag_sems.at[3], partner)
    wait_bytes(gath.at[pl.ds(0, 64)], ag_sems.at[3])
    coarse_all = rows_of(gath[...]).astype(BF)
    for i in range(4):
        lines = whole_adj[i, core].reshape(128, NC)
        kept = rows_of(gath[pl.ds(i * 32 + core * 16, 16)])
        mixed = jnp.dot(lines, coarse_all, preferred_element_type=F32) + kept
        table[core, i * 128 : (i + 1) * 128, :] = mixed.astype(BF)
    send(table.at[core], table.at[core], swap_sems.at[0], swap_sems.at[1], partner)

    for i in range(V // OUT_CHUNK):
        part = pl.ds(i * OUT_CHUNK, OUT_CHUNK)
        fine[part, :] += jnp.dot(onehot[core, part, :], table[core], preferred_element_type=F32)
    wait_bytes(table.at[0], swap_sems.at[1])
    for i in range(V // OUT_CHUNK):
        part = pl.ds(i * OUT_CHUNK, OUT_CHUNK)
        got = jnp.dot(onehot[1 - core, part, :], table[1 - core], preferred_element_type=F32)
        out[part, :] = jnp.maximum(fine[part, :] + got, 0.0).astype(BF)

    wait_bytes(core_send, core_sems.at[0])
    wait_bytes(rs_send.at[pl.ds(0, 63)], rs_sems.at[0])
    halo_wait(0)
    wait_bytes(gath.at[pl.ds(0, 63)], ag_sems.at[0])
    wait_bytes(gath.at[pl.ds(0, 64)], ag_sems.at[2])
    for stage in range(3):
        strips_wait(stage, 0)
    wait_bytes(table.at[0], swap_sems.at[0])


def per_device(
    features, w_fine, adj_tiles, tile_cols, tile_count, send_lower, send_upper, assign, w_coarse,
    coarse_adj,
):
    vmem = pl.BlockSpec(memory_space=pltpu.VMEM)
    smem = pl.BlockSpec(memory_space=pltpu.SMEM)
    hbm = pl.BlockSpec(memory_space=pl.ANY)
    dma = pltpu.SemaphoreType.DMA
    return pl.pallas_call(
        kernel,
        out_shape=pltpu.VMEM((V, F), BF),
        in_specs=[hbm, vmem, hbm, hbm, smem, smem, smem, vmem, vmem, vmem],
        out_specs=vmem,
        scratch_shapes=[
            pltpu.VMEM((NB, BS, F), BF),
            pltpu.VMEM((NB, K, BS, BS), BF),
            pltpu.VMEM((NB + 2 * H + 1, BS, F), BF),
            pltpu.VMEM((V, F), F32),
            pltpu.VMEM((2, V, NC // 2), BF),
            pltpu.VMEM((NB, BS, 128), jnp.int32),
            pltpu.VMEM((NB, 128), jnp.int32),
            pltpu.VMEM((8, NB, 128), F32),
            pltpu.VMEM((8, NB, 16, 128), BF),
            pltpu.VMEM((NB, BS, 128), BF),
            pltpu.VMEM((64, 24, 128), F32),
            pltpu.SMEM((K, NB), jnp.int32),
            pltpu.VMEM((64, 24, 128), BF),
            pltpu.VMEM((64, 24, 128), BF),
            pltpu.VMEM((64, 24, 128), BF),
            pltpu.VMEM((64, 24, 128), BF),
            pltpu.VMEM((2, H, BS, F), BF),
            pltpu.VMEM((128, 16, 128), BF),
            pltpu.VMEM((16, 128), BF),
            pltpu.VMEM((2, NC // 2, F), BF),
            pltpu.VMEM((4, 2, 4, 4, 8, NC), BF),
            dma((V // FEAT_CHUNK,)),
            dma((NB // ADJ_CHUNK,)),
            dma,
            dma((2,)),
            dma((2,)),
            dma((2, 2, 2)),
            dma((4,)),
            dma((3, 3, 2)),
            dma((2,)),
        ],
        compiler_params=pltpu.CompilerParams(
            collective_id=0, has_side_effects=True, vmem_limit_bytes=52 * 1024 * 1024
        ),
    )(
        features.reshape(NB, BS, F), w_fine, adj_tiles, tile_cols.T, tile_count, send_lower, send_upper,
        assign.reshape(NB, BS), w_coarse, coarse_adj,
    )


def solution(mesh):
    both = ("dom", "grp")
    placed = (
        P(both, None), P(), P(both, None, None, None), P(both, None), P(both), P(both), P(both),
        P(both), P(), P(both, None),
    )
    return jax.shard_map(
        per_device, mesh=mesh, in_specs=placed, out_specs=P(both, None), check_vma=False
    )
```

```python
import jax
import jax.numpy as jnp
from jax import lax
from jax.experimental import pallas as pl
from jax.experimental.pallas import tpu as pltpu
from jax.sharding import PartitionSpec as P

MESH = pl.DeviceIdType.MESH
F = 256
BS = 128
K = 20
H = 4
NC = 1024
V = 4096
NB = 32
BF = jnp.bfloat16
F32 = jnp.float32
ADJ_CHUNK = 4
FEAT_CHUNK = 1024
OUT_CHUNK = 512
STRIPS = (
    (0, 384, ("x", "y", "z")), (384, 384, ("x", "z", "y")), (768, 256, ("z", "y", "x")),
)
DEAD = NB + 2 * H


def ring_hops(d):
    return min(d % 4, -d % 4)


OFFSETS = sorted(
    [
        (ox, oz, oy)
        for ox in range(4)
        for oz in range(4)
        for oy in range(4)
        if (ox, oz, oy) != (0, 0, 0)
    ],
    key=lambda o: -sum(ring_hops(d) for d in o),
)


def wait_bytes(ref, sem):
    pltpu.make_async_copy(ref, ref, sem).wait()


def send(src, dst, ssem, rsem, to):
    pltpu.make_async_remote_copy(
        src, dst, ssem, rsem, device_id=to, device_id_type=MESH
    ).start()


def rows_of(pieces):
    wide = pieces.astype(F32)
    n = wide.shape[0]
    low = wide[:, :8, :].reshape(n * 8, 128)
    high = wide[:, 8:16, :].reshape(n * 8, 128)
    return jnp.concatenate([low, high], axis=1)


def piece_of(rows):
    return jnp.concatenate([rows[:, :128], rows[:, 128:]], axis=0).astype(BF)


def kernel(
    feat_hbm, wf_ref, adj_hbm, cols_hbm, live_ref, lower_ref, upper_ref, assign_ref, wc_ref,
    cadj_ref, out,
    feat, adj, ext, fine, onehot, acol, low, match, match16, hit, mine, cols, core_send, core_recv, rs_send, rs_recv,
    halo, gath, own_piece, table, whole_adj,
    feat_sem, adj_sem, cols_sem, core_sems, rs_sems, halo_sems, ag_sems, strip_sems, swap_sems,
):
    dom = lax.axis_index("dom")
    grp = lax.axis_index("grp")
    x, core = dom // 2, dom % 2
    z, y = grp // 4, grp % 4
    chip = x * 16 + grp
    place = dom * 16 + grp

    def chip_at(o):
        return (x + o[0]) % 4, ((z + o[1]) % 4) * 4 + (y + o[2]) % 4

    def same_core(o):
        to_x, to_grp = chip_at(o)
        return {"dom": to_x * 2 + core, "grp": to_grp}

    partner = {"dom": x * 2 + 1 - core, "grp": grp}
    upper = {"dom": (dom + 1) % 8, "grp": grp}
    lower = {"dom": (dom + 7) % 8, "grp": grp}
    across = {"dom": (dom + core * 2 + 7) % 8, "grp": grp}

    feat_copies = []
    for i in range(V // FEAT_CHUNK):
        part = pl.ds(i * FEAT_CHUNK // BS, FEAT_CHUNK // BS)
        c = pltpu.make_async_copy(feat_hbm.at[part], feat.at[part], feat_sem.at[i])
        c.start()
        feat_copies.append(c)
    barrier = pltpu.get_barrier_semaphore()
    for o in OFFSETS:
        pl.semaphore_signal(barrier, inc=1, device_id=same_core(o), device_id_type=MESH)
    pl.semaphore_signal(barrier, inc=1, device_id=partner, device_id_type=MESH)
    pl.semaphore_signal(barrier, inc=1, device_id=across, device_id_type=MESH)
    cols_copy = pltpu.make_async_copy(cols_hbm, cols, cols_sem)
    cols_copy.start()
    adj_copies = []
    for i in range(NB // ADJ_CHUNK):
        part = pl.ds(i * ADJ_CHUNK, ADJ_CHUNK)
        c = pltpu.make_async_copy(adj_hbm.at[part], adj.at[part], adj_sem.at[i])
        c.start()
        adj_copies.append(c)

    whole_adj[x, core, z, y] = cadj_ref[...]
    spot = {"x": x, "z": z, "y": y}

    def region(free, strip, most=None):
        at = [pl.ds(0, 4) if a in free else spot[a] for a in ("x", "z", "y")]
        return whole_adj.at[at[0], core, at[1], at[2], :, pl.ds(strip[0], strip[1])]

    def strips_go(stage):
        for i, strip in enumerate(STRIPS):
            free, axis = strip[2][:stage], strip[2][stage]
            part = region(free, strip)
            for step in (2, 1, 3):
                o = [step if a == axis else 0 for a in ("x", "z", "y")]
                send(part, part, strip_sems.at[i, stage, 0], strip_sems.at[i, stage, 1], same_core(o))

    def strips_wait(stage, way):
        for i, strip in enumerate(STRIPS):
            cut = pl.ds(strip[0], strip[1])
            if stage == 0:
                three = whole_adj.at[0, 0, 0, pl.ds(0, 3), :, cut]
            elif stage == 1:
                three = whole_adj.at[0, 0, pl.ds(0, 3), pl.ds(0, 4), :, cut]
            else:
                three = whole_adj.at[pl.ds(0, 3), 0, pl.ds(0, 4), pl.ds(0, 4), :, cut]
            wait_bytes(three, strip_sems.at[i, stage, way])

    def halo_parts(part):
        first = part * (H // 2)
        for side, base in ((0, NB + H), (1, NB)):
            yield side, pl.ds(first, H // 2), pl.ds(base + first, H // 2)

    def halo_go(part):
        for side, src, dst in halo_parts(part):
            send(
                halo.at[side, src], ext.at[dst], halo_sems.at[part, side, 0],
                halo_sems.at[part, side, 1], (lower, upper)[side],
            )

    def halo_wait(way):
        for part in range(2):
            for side, src, dst in halo_parts(part):
                wait_bytes(ext.at[dst], halo_sems.at[part, side, way])

    nodes = assign_ref[...]
    low[...] = nodes & 127
    for m in range(NC // 128):
        match[m] = jnp.where((nodes >> 7) == m, 1.0, 0.0)
    seat = lax.broadcasted_iota(jnp.int32, (BS, 128), 0)

    def hits_of(b, carry):
        hit[b] = jnp.where(low[pl.ds(b, 1), :] == seat, 1.0, 0.0).astype(BF)
        for m in range(NC // 128):
            row = match[m, pl.ds(b, 1), :]
            match16[m, b] = jnp.broadcast_to(row, (16, 128)).astype(BF)
        return carry

    lax.fori_loop(0, NB, hits_of, 0, unroll=4)
    for c in feat_copies:
        c.wait()

    def segment_half(which, put):
        for g in range(2):
            total = jnp.zeros((256, F), F32)
            counts = [jnp.zeros((128, 128), BF) for _ in range(2)]
            for t in range(V // 256):
                strips = []
                for i in range(2):
                    m = 4 * g + 2 * i + which
                    pair = []
                    for b in (2 * t, 2 * t + 1):
                        one = hit[b] * jnp.concatenate([match16[m, b]] * 8, axis=0)
                        counts[i] = counts[i] + one
                        pair.append(one)
                    strips.append(jnp.concatenate(pair, axis=1))
                total = total + jnp.dot(
                    jnp.concatenate(strips, axis=0),
                    feat[pl.ds(2 * t, 2)].reshape(256, F),
                    preferred_element_type=F32,
                )
            count = jnp.dot(
                jnp.concatenate(counts, axis=0), jnp.ones((128, 128), BF),
                preferred_element_type=F32,
            )
            sums = total.reshape(32, 8, F)
            put(
                pl.ds(32 * g, 32),
                jnp.concatenate(
                    [sums[:, :, :128], sums[:, :, 128:], count.reshape(32, 8, 128)], axis=1
                ),
            )

    def put_send(part, value):
        core_send[part] = value.astype(BF)

    def put_mine(part, value):
        mine[part] = value

    segment_half(1 - core, put_send)
    for i in range(H):
        for side, ref in enumerate((lower_ref, upper_ref)):
            block = feat[ref[i]]
            halo[side, i] = jnp.dot(block, wf_ref[...], preferred_element_type=F32).astype(BF)
    pl.semaphore_wait(barrier, len(OFFSETS) + 2)
    strips_go(0)
    send(core_send, core_recv, core_sems.at[0], core_sems.at[1], partner)
    halo_go(0)
    segment_half(core, put_mine)
    wait_bytes(core_recv, core_sems.at[1])
    rs_send[...] = (mine[...] + core_recv[...].astype(F32)).astype(BF)
    for o in OFFSETS:
        to_x, to_grp = chip_at(o)
        send(
            rs_send.at[to_x * 16 + to_grp], rs_recv.at[chip], rs_sems.at[0], rs_sems.at[1],
            same_core(o),
        )
    rs_recv[chip] = rs_send[chip]

    def project(i, carry):
        block = feat[pl.ds(i * 4, 4)].reshape(512, F)
        rows = jnp.dot(block, wf_ref[...], preferred_element_type=F32).astype(BF)
        ext[pl.ds(i * 4, 4)] = rows.reshape(4, BS, F)
        return carry

    lax.fori_loop(0, V // 512, project, 0, unroll=4)
    ext[DEAD] = jnp.zeros((BS, F), BF)

    strips_wait(0, 1)
    strips_go(1)
    halo_go(1)
    turned = nodes.astype(F32).T
    for r in range(NB):
        acol[r] = jnp.broadcast_to(turned[:, r : r + 1], (BS, 128)).astype(jnp.int32)
    lanes = lax.broadcasted_iota(jnp.int32, (BS, 128), 1)

    def spread(r, carry):
        apart = acol[r] - lanes
        tile = jnp.where((apart & 127) == 0, apart >> 7, -1).astype(F32).astype(BF)
        one, none = jnp.ones((BS, 128), BF), jnp.zeros((BS, 128), BF)
        for j in range(NC // 128):
            lanes_of = pl.ds(j // 2 * 128, 128)
            onehot[j % 2, pl.ds(pl.multiple_of(r * BS, BS), BS), lanes_of] = jnp.where(
                tile == j, one, none
            )
        return carry

    lax.fori_loop(0, NB, spread, 0, unroll=4)

    def pick(r, k):
        live = jnp.minimum(jnp.maximum(live_ref[r] - k, 0), 1)
        return DEAD + (cols[k, r] - DEAD) * live

    def spmm(r, carry):
        total = jnp.zeros((BS, F), F32)
        for k in range(0, K, 2):
            tiles = jnp.concatenate([adj[r, k], adj[r, k + 1]], axis=1)
            blocks = jnp.concatenate([ext[pick(r, k)], ext[pick(r, k + 1)]], axis=0)
            total = total + jnp.dot(tiles, blocks, preferred_element_type=F32)
        fine[pl.ds(pl.multiple_of(r * BS, BS), BS), :] = total
        return carry

    wait_bytes(rs_recv.at[pl.ds(0, 63)], rs_sems.at[1])
    whole = jnp.sum(rs_recv[...].astype(F32), axis=0)
    root = jnp.sqrt(whole[16:24, :])
    coarse = jnp.concatenate([whole[:8, :] / root, whole[8:16, :] / root], axis=1).astype(BF)
    projected = jnp.dot(coarse, wc_ref[...], preferred_element_type=F32)
    own_piece[...] = piece_of(projected)
    gath[place] = own_piece[...]
    for o in OFFSETS:
        send(own_piece, gath.at[place], ag_sems.at[0], ag_sems.at[4 + o[0]], same_core(o))
    strips_wait(1, 1)
    strips_go(2)
    halo_wait(1)
    for i in range(4):
        adj_copies[i].wait()
    cols_copy.wait()
    lax.fori_loop(0, 16, spmm, 0, unroll=8)

    for i in range(4, 8):
        adj_copies[i].wait()
    lax.fori_loop(16, 32, spmm, 0, unroll=8)
    for ox in (0, 1, 3, 2):
        wait_bytes(gath.at[pl.ds(0, 16 if ox else 15)], ag_sems.at[4 + ox])
        part = gath.at[pl.ds((x + 4 - ox) % 4 * 32 + core * 16, 16)]
        send(part, part, ag_sems.at[2], ag_sems.at[3], partner)
    strips_wait(2, 1)
    wait_bytes(gath.at[pl.ds(0, 64)], ag_sems.at[3])
    coarse_all = rows_of(gath[...]).astype(BF)
    for i in range(4):
        lines = whole_adj[i, core].reshape(128, NC)
        kept = rows_of(gath[pl.ds(i * 32 + core * 16, 16)])
        mixed = jnp.dot(lines, coarse_all, preferred_element_type=F32) + kept
        table[core, i * 128 : (i + 1) * 128, :] = mixed.astype(BF)
    send(table.at[core], table.at[core], swap_sems.at[0], swap_sems.at[1], partner)

    for i in range(V // OUT_CHUNK):
        part = pl.ds(i * OUT_CHUNK, OUT_CHUNK)
        fine[part, :] += jnp.dot(onehot[core, part, :], table[core], preferred_element_type=F32)
    wait_bytes(table.at[0], swap_sems.at[1])
    for i in range(V // OUT_CHUNK):
        part = pl.ds(i * OUT_CHUNK, OUT_CHUNK)
        got = jnp.dot(onehot[1 - core, part, :], table[1 - core], preferred_element_type=F32)
        out[part, :] = jnp.maximum(fine[part, :] + got, 0.0).astype(BF)

    wait_bytes(core_send, core_sems.at[0])
    wait_bytes(rs_send.at[pl.ds(0, 63)], rs_sems.at[0])
    halo_wait(0)
    wait_bytes(gath.at[pl.ds(0, 63)], ag_sems.at[0])
    wait_bytes(gath.at[pl.ds(0, 64)], ag_sems.at[2])
    for stage in range(3):
        strips_wait(stage, 0)
    wait_bytes(table.at[0], swap_sems.at[0])


def per_device(
    features, w_fine, adj_tiles, tile_cols, tile_count, send_lower, send_upper, assign, w_coarse,
    coarse_adj,
):
    vmem = pl.BlockSpec(memory_space=pltpu.VMEM)
    smem = pl.BlockSpec(memory_space=pltpu.SMEM)
    hbm = pl.BlockSpec(memory_space=pl.ANY)
    dma = pltpu.SemaphoreType.DMA
    return pl.pallas_call(
        kernel,
        out_shape=pltpu.VMEM((V, F), BF),
        in_specs=[hbm, vmem, hbm, hbm, smem, smem, smem, vmem, vmem, vmem],
        out_specs=vmem,
        scratch_shapes=[
            pltpu.VMEM((NB, BS, F), BF),
            pltpu.VMEM((NB, K, BS, BS), BF),
            pltpu.VMEM((NB + 2 * H + 1, BS, F), BF),
            pltpu.VMEM((V, F), F32),
            pltpu.VMEM((2, V, NC // 2), BF),
            pltpu.VMEM((NB, BS, 128), jnp.int32),
            pltpu.VMEM((NB, 128), jnp.int32),
            pltpu.VMEM((8, NB, 128), F32),
            pltpu.VMEM((8, NB, 16, 128), BF),
            pltpu.VMEM((NB, BS, 128), BF),
            pltpu.VMEM((64, 24, 128), F32),
            pltpu.SMEM((K, NB), jnp.int32),
            pltpu.VMEM((64, 24, 128), BF),
            pltpu.VMEM((64, 24, 128), BF),
            pltpu.VMEM((64, 24, 128), BF),
            pltpu.VMEM((64, 24, 128), BF),
            pltpu.VMEM((2, H, BS, F), BF),
            pltpu.VMEM((128, 16, 128), BF),
            pltpu.VMEM((16, 128), BF),
            pltpu.VMEM((2, NC // 2, F), BF),
            pltpu.VMEM((4, 2, 4, 4, 8, NC), BF),
            dma((V // FEAT_CHUNK,)),
            dma((NB // ADJ_CHUNK,)),
            dma,
            dma((2,)),
            dma((2,)),
            dma((2, 2, 2)),
            dma((8,)),
            dma((3, 3, 2)),
            dma((2,)),
        ],
        compiler_params=pltpu.CompilerParams(
            collective_id=0, has_side_effects=True, vmem_limit_bytes=52 * 1024 * 1024
        ),
    )(
        features.reshape(NB, BS, F), w_fine, adj_tiles, tile_cols.T, tile_count, send_lower, send_upper,
        assign.reshape(NB, BS), w_coarse, coarse_adj,
    )


def solution(mesh):
    both = ("dom", "grp")
    placed = (
        P(both, None), P(), P(both, None, None, None), P(both, None), P(both), P(both), P(both),
        P(both), P(), P(both, None),
    )
    return jax.shard_map(
        per_device, mesh=mesh, in_specs=placed, out_specs=P(both, None), check_vma=False
    )
```

```python
import jax
import jax.numpy as jnp
from jax import lax
from jax.experimental import pallas as pl
from jax.experimental.pallas import tpu as pltpu
from jax.sharding import PartitionSpec as P

MESH = pl.DeviceIdType.MESH
F = 256
BS = 128
K = 20
H = 4
NC = 1024
V = 4096
NB = 32
BF = jnp.bfloat16
F32 = jnp.float32
ADJ_CHUNK = 4
FEAT_CHUNK = 1024
OUT_CHUNK = 512
STRIPS = (
    (0, 256, ("z", "y", "x")), (256, 384, ("x", "y", "z")), (640, 384, ("x", "z", "y")),
)
DEAD = NB + 2 * H


def ring_hops(d):
    return min(d % 4, -d % 4)


OFFSETS = sorted(
    [
        (ox, oz, oy)
        for ox in range(4)
        for oz in range(4)
        for oy in range(4)
        if (ox, oz, oy) != (0, 0, 0)
    ],
    key=lambda o: -sum(ring_hops(d) for d in o),
)


def wait_bytes(ref, sem):
    pltpu.make_async_copy(ref, ref, sem).wait()


def send(src, dst, ssem, rsem, to):
    pltpu.make_async_remote_copy(
        src, dst, ssem, rsem, device_id=to, device_id_type=MESH
    ).start()


def rows_of(pieces):
    wide = pieces.astype(F32)
    n = wide.shape[0]
    low = wide[:, :8, :].reshape(n * 8, 128)
    high = wide[:, 8:16, :].reshape(n * 8, 128)
    return jnp.concatenate([low, high], axis=1)


def piece_of(rows):
    return jnp.concatenate([rows[:, :128], rows[:, 128:]], axis=0).astype(BF)


def kernel(
    feat_hbm, wf_ref, adj_hbm, cols_hbm, live_ref, lower_ref, upper_ref, assign_ref, wc_ref,
    cadj_ref, out,
    feat, adj, ext, fine, onehot, acol, low, match, match16, hit, mine, cols, core_send, core_recv, rs_send, rs_recv,
    halo, gath, own_piece, table, whole_adj, coarse, sums,
    feat_sem, adj_sem, cols_sem, core_sems, rs_sems, halo_sems, ag_sems, strip_sems, swap_sems,
):
    dom = lax.axis_index("dom")
    grp = lax.axis_index("grp")
    x, core = dom // 2, dom % 2
    z, y = grp // 4, grp % 4
    chip = x * 16 + grp
    place = dom * 16 + grp

    def chip_at(o):
        return (x + o[0]) % 4, ((z + o[1]) % 4) * 4 + (y + o[2]) % 4

    def same_core(o):
        to_x, to_grp = chip_at(o)
        return {"dom": to_x * 2 + core, "grp": to_grp}

    partner = {"dom": x * 2 + 1 - core, "grp": grp}
    upper = {"dom": (dom + 1) % 8, "grp": grp}
    lower = {"dom": (dom + 7) % 8, "grp": grp}
    across = {"dom": (dom + core * 2 + 7) % 8, "grp": grp}

    feat_copies = []
    for i in range(V // FEAT_CHUNK):
        part = pl.ds(i * FEAT_CHUNK // BS, FEAT_CHUNK // BS)
        c = pltpu.make_async_copy(feat_hbm.at[part], feat.at[part], feat_sem.at[i])
        c.start()
        feat_copies.append(c)
    barrier = pltpu.get_barrier_semaphore()
    for o in OFFSETS:
        pl.semaphore_signal(barrier, inc=1, device_id=same_core(o), device_id_type=MESH)
    pl.semaphore_signal(barrier, inc=1, device_id=partner, device_id_type=MESH)
    pl.semaphore_signal(barrier, inc=1, device_id=across, device_id_type=MESH)
    cols_copy = pltpu.make_async_copy(cols_hbm, cols, cols_sem)
    cols_copy.start()
    adj_copies = []
    for i in range(NB // ADJ_CHUNK):
        part = pl.ds(i * ADJ_CHUNK, ADJ_CHUNK)
        c = pltpu.make_async_copy(adj_hbm.at[part], adj.at[part], adj_sem.at[i])
        c.start()
        adj_copies.append(c)

    whole_adj[x, core, z, y] = cadj_ref[...]
    spot = {"x": x, "z": z, "y": y}

    def region(free, strip, most=None):
        at = [pl.ds(0, 4) if a in free else spot[a] for a in ("x", "z", "y")]
        return whole_adj.at[at[0], core, at[1], at[2], :, pl.ds(strip[0], strip[1])]

    def strips_go(stage):
        for i, strip in enumerate(STRIPS):
            free, axis = strip[2][:stage], strip[2][stage]
            part = region(free, strip)
            for step in (2, 1, 3):
                o = [step if a == axis else 0 for a in ("x", "z", "y")]
                send(part, part, strip_sems.at[i, stage, 0], strip_sems.at[i, stage, 1], same_core(o))

    def strip_wait(i, stage, way):
        cut = pl.ds(STRIPS[i][0], STRIPS[i][1])
        if stage == 0:
            three = whole_adj.at[0, 0, 0, pl.ds(0, 3), :, cut]
        elif stage == 1:
            three = whole_adj.at[0, 0, pl.ds(0, 3), pl.ds(0, 4), :, cut]
        else:
            three = whole_adj.at[pl.ds(0, 3), 0, pl.ds(0, 4), pl.ds(0, 4), :, cut]
        wait_bytes(three, strip_sems.at[i, stage, way])

    def strips_wait(stage, way):
        for i in range(len(STRIPS)):
            strip_wait(i, stage, way)

    def halo_parts(part):
        first = part * (H // 2)
        for side, base in ((0, NB + H), (1, NB)):
            yield side, pl.ds(first, H // 2), pl.ds(base + first, H // 2)

    def halo_go(part):
        for side, src, dst in halo_parts(part):
            send(
                halo.at[side, src], ext.at[dst], halo_sems.at[part, side, 0],
                halo_sems.at[part, side, 1], (lower, upper)[side],
            )

    def halo_wait(way):
        for part in range(2):
            for side, src, dst in halo_parts(part):
                wait_bytes(ext.at[dst], halo_sems.at[part, side, way])

    nodes = assign_ref[...]
    low[...] = nodes & 127
    for m in range(NC // 128):
        match[m] = jnp.where((nodes >> 7) == m, 1.0, 0.0)
    seat = lax.broadcasted_iota(jnp.int32, (BS, 128), 0)

    def hits_of(b, carry):
        hit[b] = jnp.where(low[pl.ds(b, 1), :] == seat, 1.0, 0.0).astype(BF)
        for m in range(NC // 128):
            row = match[m, pl.ds(b, 1), :]
            match16[m, b] = jnp.broadcast_to(row, (16, 128)).astype(BF)
        return carry

    lax.fori_loop(0, NB, hits_of, 0, unroll=4)
    for c in feat_copies:
        c.wait()

    def segment_half(which, put):
        for g in range(2):
            total = jnp.zeros((256, F), F32)
            counts = [jnp.zeros((128, 128), BF) for _ in range(2)]
            for t in range(V // 256):
                strips = []
                for i in range(2):
                    m = 4 * g + 2 * i + which
                    pair = []
                    for b in (2 * t, 2 * t + 1):
                        one = hit[b] * jnp.concatenate([match16[m, b]] * 8, axis=0)
                        counts[i] = counts[i] + one
                        pair.append(one)
                    strips.append(jnp.concatenate(pair, axis=1))
                total = total + jnp.dot(
                    jnp.concatenate(strips, axis=0),
                    feat[pl.ds(2 * t, 2)].reshape(256, F),
                    preferred_element_type=F32,
                )
            count = jnp.dot(
                jnp.concatenate(counts, axis=0), jnp.ones((128, 128), BF),
                preferred_element_type=F32,
            )
            sums = total.reshape(32, 8, F)
            put(
                pl.ds(32 * g, 32),
                jnp.concatenate(
                    [sums[:, :, :128], sums[:, :, 128:], count.reshape(32, 8, 128)], axis=1
                ),
            )

    def put_send(part, value):
        core_send[part] = value.astype(BF)

    def put_mine(part, value):
        mine[part] = value

    segment_half(1 - core, put_send)
    for i in range(H):
        for side, ref in enumerate((lower_ref, upper_ref)):
            block = feat[ref[i]]
            halo[side, i] = jnp.dot(block, wf_ref[...], preferred_element_type=F32).astype(BF)
    pl.semaphore_wait(barrier, len(OFFSETS) + 2)
    strips_go(0)
    send(core_send, core_recv, core_sems.at[0], core_sems.at[1], partner)
    halo_go(0)
    segment_half(core, put_mine)
    wait_bytes(core_recv, core_sems.at[1])
    rs_send[...] = (mine[...] + core_recv[...].astype(F32)).astype(BF)
    for o in OFFSETS:
        to_x, to_grp = chip_at(o)
        send(
            rs_send.at[to_x * 16 + to_grp], rs_recv.at[chip], rs_sems.at[0], rs_sems.at[1],
            same_core(o),
        )
    rs_recv[chip] = rs_send[chip]

    def project(i, carry):
        block = feat[pl.ds(i * 4, 4)].reshape(512, F)
        rows = jnp.dot(block, wf_ref[...], preferred_element_type=F32).astype(BF)
        ext[pl.ds(i * 4, 4)] = rows.reshape(4, BS, F)
        return carry

    lax.fori_loop(0, V // 512, project, 0, unroll=4)
    ext[DEAD] = jnp.zeros((BS, F), BF)

    strips_wait(0, 1)
    strips_go(1)
    halo_go(1)
    turned = nodes.astype(F32).T
    for r in range(NB):
        acol[r] = jnp.broadcast_to(turned[:, r : r + 1], (BS, 128)).astype(jnp.int32)
    lanes = lax.broadcasted_iota(jnp.int32, (BS, 128), 1)

    def spread(r, carry):
        apart = acol[r] - lanes
        tile = jnp.where((apart & 127) == 0, apart >> 7, -1).astype(F32).astype(BF)
        one, none = jnp.ones((BS, 128), BF), jnp.zeros((BS, 128), BF)
        for j in range(NC // 128):
            lanes_of = pl.ds(j // 2 * 128, 128)
            onehot[j % 2, pl.ds(pl.multiple_of(r * BS, BS), BS), lanes_of] = jnp.where(
                tile == j, one, none
            )
        return carry

    lax.fori_loop(0, NB, spread, 0, unroll=4)

    def pick(r, k):
        live = jnp.minimum(jnp.maximum(live_ref[r] - k, 0), 1)
        return DEAD + (cols[k, r] - DEAD) * live

    def spmm(r, carry):
        total = jnp.zeros((BS, F), F32)
        for k in range(0, K, 2):
            tiles = jnp.concatenate([adj[r, k], adj[r, k + 1]], axis=1)
            blocks = jnp.concatenate([ext[pick(r, k)], ext[pick(r, k + 1)]], axis=0)
            total = total + jnp.dot(tiles, blocks, preferred_element_type=F32)
        fine[pl.ds(pl.multiple_of(r * BS, BS), BS), :] = total
        return carry

    wait_bytes(rs_recv.at[pl.ds(0, 63)], rs_sems.at[1])
    whole = jnp.sum(rs_recv[...].astype(F32), axis=0)
    root = jnp.sqrt(whole[16:24, :])
    scaled = jnp.concatenate([whole[:8, :] / root, whole[8:16, :] / root], axis=1).astype(BF)
    projected = jnp.dot(scaled, wc_ref[...], preferred_element_type=F32)
    own_piece[...] = piece_of(projected)
    gath[place] = own_piece[...]
    for o in OFFSETS:
        send(own_piece, gath.at[place], ag_sems.at[0], ag_sems.at[4 + o[0]], same_core(o))
    strips_wait(1, 1)
    strips_go(2)
    halo_wait(1)
    for i in range(4):
        adj_copies[i].wait()
    cols_copy.wait()
    lax.fori_loop(0, 16, spmm, 0, unroll=8)

    for i in range(4, 8):
        adj_copies[i].wait()
    lax.fori_loop(16, 32, spmm, 0, unroll=8)
    for ox in (0, 1, 3, 2):
        wait_bytes(gath.at[pl.ds(0, 16 if ox else 15)], ag_sems.at[4 + ox])
        part = gath.at[pl.ds((x + 4 - ox) % 4 * 32 + core * 16, 16)]
        send(part, part, ag_sems.at[2], ag_sems.at[3], partner)
    wait_bytes(gath.at[pl.ds(0, 64)], ag_sems.at[3])
    coarse[...] = rows_of(gath[...]).astype(BF)
    for i in range(4):
        sums[i] = rows_of(gath[pl.ds(i * 32 + core * 16, 16)])
    for n, (start, width, _) in enumerate(STRIPS):
        strip_wait(n, 2, 1)
        for i in range(4):
            lines = whole_adj[i, core, :, :, :, start : start + width].reshape(128, width)
            total = sums[i] + jnp.dot(
                lines, coarse[start : start + width, :], preferred_element_type=F32
            )
            if n < 2:
                sums[i] = total
            else:
                table[core, i * 128 : (i + 1) * 128, :] = total.astype(BF)
    send(table.at[core], table.at[core], swap_sems.at[0], swap_sems.at[1], partner)

    for i in range(V // OUT_CHUNK):
        part = pl.ds(i * OUT_CHUNK, OUT_CHUNK)
        fine[part, :] += jnp.dot(onehot[core, part, :], table[core], preferred_element_type=F32)
    wait_bytes(table.at[0], swap_sems.at[1])
    for i in range(V // OUT_CHUNK):
        part = pl.ds(i * OUT_CHUNK, OUT_CHUNK)
        got = jnp.dot(onehot[1 - core, part, :], table[1 - core], preferred_element_type=F32)
        out[part, :] = jnp.maximum(fine[part, :] + got, 0.0).astype(BF)

    wait_bytes(core_send, core_sems.at[0])
    wait_bytes(rs_send.at[pl.ds(0, 63)], rs_sems.at[0])
    halo_wait(0)
    wait_bytes(gath.at[pl.ds(0, 63)], ag_sems.at[0])
    wait_bytes(gath.at[pl.ds(0, 64)], ag_sems.at[2])
    for stage in range(3):
        strips_wait(stage, 0)
    wait_bytes(table.at[0], swap_sems.at[0])


def per_device(
    features, w_fine, adj_tiles, tile_cols, tile_count, send_lower, send_upper, assign, w_coarse,
    coarse_adj,
):
    vmem = pl.BlockSpec(memory_space=pltpu.VMEM)
    smem = pl.BlockSpec(memory_space=pltpu.SMEM)
    hbm = pl.BlockSpec(memory_space=pl.ANY)
    dma = pltpu.SemaphoreType.DMA
    return pl.pallas_call(
        kernel,
        out_shape=pltpu.VMEM((V, F), BF),
        in_specs=[hbm, vmem, hbm, hbm, smem, smem, smem, vmem, vmem, vmem],
        out_specs=vmem,
        scratch_shapes=[
            pltpu.VMEM((NB, BS, F), BF),
            pltpu.VMEM((NB, K, BS, BS), BF),
            pltpu.VMEM((NB + 2 * H + 1, BS, F), BF),
            pltpu.VMEM((V, F), F32),
            pltpu.VMEM((2, V, NC // 2), BF),
            pltpu.VMEM((NB, BS, 128), jnp.int32),
            pltpu.VMEM((NB, 128), jnp.int32),
            pltpu.VMEM((8, NB, 128), F32),
            pltpu.VMEM((8, NB, 16, 128), BF),
            pltpu.VMEM((NB, BS, 128), BF),
            pltpu.VMEM((64, 24, 128), F32),
            pltpu.SMEM((K, NB), jnp.int32),
            pltpu.VMEM((64, 24, 128), BF),
            pltpu.VMEM((64, 24, 128), BF),
            pltpu.VMEM((64, 24, 128), BF),
            pltpu.VMEM((64, 24, 128), BF),
            pltpu.VMEM((2, H, BS, F), BF),
            pltpu.VMEM((128, 16, 128), BF),
            pltpu.VMEM((16, 128), BF),
            pltpu.VMEM((2, NC // 2, F), BF),
            pltpu.VMEM((4, 2, 4, 4, 8, NC), BF),
            pltpu.VMEM((NC, F), BF),
            pltpu.VMEM((4, 128, F), F32),
            dma((V // FEAT_CHUNK,)),
            dma((NB // ADJ_CHUNK,)),
            dma,
            dma((2,)),
            dma((2,)),
            dma((2, 2, 2)),
            dma((8,)),
            dma((3, 3, 2)),
            dma((2,)),
        ],
        compiler_params=pltpu.CompilerParams(
            collective_id=0, has_side_effects=True, vmem_limit_bytes=52 * 1024 * 1024
        ),
    )(
        features.reshape(NB, BS, F), w_fine, adj_tiles, tile_cols.T, tile_count, send_lower, send_upper,
        assign.reshape(NB, BS), w_coarse, coarse_adj,
    )


def solution(mesh):
    both = ("dom", "grp")
    placed = (
        P(both, None), P(), P(both, None, None, None), P(both, None), P(both), P(both), P(both),
        P(both), P(), P(both, None),
    )
    return jax.shard_map(
        per_device, mesh=mesh, in_specs=placed, out_specs=P(both, None), check_vma=False
    )
```
